32 devices in a mesh: dom: 8 (over y, x, core), feat: 4 (over z).
Axes of the slice: x: 2, y: 2, z: 4, core: 2. Of those that a mesh axis runs over, the one named last changes fastest.
Arguments:
- features: bfloat16 [512, 65536], P('feat', 'dom'), may hold values from -3 to 3
- send_blocks: int32 [8, 8, 8], P('dom'), may hold values from 0 to 63, as said below
- counts: int32 [8, 8], P('dom'), may hold values from 0 to 8, as said below
- tile_blocks: int32 [24, 512], P(None, 'dom'), may hold values from 0 to 127, as said below
- neighbours: int32 [24, 65536], P(None, 'dom'), may hold values from 0 to 127
- degree: int32 [65536], P('dom'), may hold values from 1 to 24
- epsilon: float32 [1], replicated, may hold values from -0.3 to 0.6
- w_first: bfloat16 [512, 512], replicated, may hold values from -0.25 to 0.25
- b_first: float32 [512], replicated, may hold values from -3 to 3
- w_second: bfloat16 [512, 512], replicated, may hold values from -0.25 to 0.25
- b_second: float32 [512], replicated, may hold values from -3 to 3
Outputs:
- updated: bfloat16 [65536, 512], P(('dom', 'feat'))
The draws below stay inside these ranges and needn't reach their ends.
Inputs may be any that keep to these rules, and one draw needn't show every extreme that they name: `send_blocks`: entry [q, p, s] is a row block of partition q; the entries of one pair (q, p) are distinct. counts[q, p] leading slots of send_blocks[q, p] are used; zero where q == p; in every draw some partition receives 8 blocks from every other partition. `tile_blocks`: an entry for a row block of partition p is below 64 (a row block of p) or equals 64 + q * 8 + s for a slot s of a partition q other than p.
All inputs are finite; a program needn't handle non-finite values.
Results may differ from the reference program's by a relative error of at most 0.0055.
Values may be sent and summed in bfloat16 or wider, within the bound.
A program may use at most 64 MiB of HBM per device.

```python
import jax
import jax.numpy as jnp
from jax import lax

D = 512
H = 512
ROWS = 8192
BLOCK = 128
SLOTS = 8
NEIGH = 24
PARTITIONS = 8
NODES = 65536
BLOCKS = 64


def draw_send_blocks(key, part):
    key_list = jax.random.split(jax.random.fold_in(key, 11), PARTITIONS * PARTITIONS)

    def pick(single):
        return jax.random.permutation(single, BLOCKS)[:SLOTS]
    picked = jax.vmap(pick)(key_list)
    return picked.reshape(PARTITIONS, PARTITIONS, SLOTS).astype(jnp.int32)


def draw_counts(key, part):
    first, second = jax.random.split(jax.random.fold_in(key, 23))
    base = jax.random.randint(first, (PARTITIONS, PARTITIONS), 1, SLOTS + 1)
    heavy = jax.random.randint(second, (), 0, PARTITIONS)
    column = jnp.arange(PARTITIONS, dtype=jnp.int32)[None, :]
    rowpos = jnp.arange(PARTITIONS, dtype=jnp.int32)[:, None]
    base = jnp.where(column == heavy, SLOTS, base)
    base = jnp.where(column == rowpos, 0, base)
    return base.astype(jnp.int32)


def draw_tile_blocks(key, part):
    keys = jax.random.split(jax.random.fold_in(key, 37), 4)
    block_count = NODES // BLOCK
    shape = (block_count, NEIGH)
    dst_part = (jnp.arange(block_count, dtype=jnp.int32) // BLOCKS)[:, None]
    which = jax.random.randint(keys[0], shape, 0, 2)
    local = jax.random.randint(keys[1], shape, 0, BLOCKS)
    source = (dst_part + jax.random.randint(keys[2], shape, 1, PARTITIONS)) % PARTITIONS
    slot_pick = jax.random.randint(keys[3], shape, 0, SLOTS)
    remote = BLOCKS + source * SLOTS + slot_pick
    return jnp.where(which == 0, local, remote).astype(jnp.int32).T


def set_ends(entries, key, least, high):
    spot = [jax.random.randint(jax.random.fold_in(key, axis), (), 0, length) for axis, length in enumerate(entries.shape)]
    longest = entries.shape.index(max(entries.shape))
    beside = spot[:longest] + [(spot[longest] + 1) % entries.shape[longest]] + spot[longest + 1:]
    return entries.at[tuple(spot)].set(least).at[tuple(beside)].set(high)


def block_levels(rng, dims, pieces, low, largest):
    gain = 1.0
    for dim, shards_of in pieces:
        draws = jax.random.uniform(jax.random.fold_in(jax.random.fold_in(rng, 6), dim), (shards_of,), jnp.float32, low / len(pieces), largest / len(pieces))
        gain = gain * jnp.repeat(jnp.exp(draws), dims[dim] // shards_of).reshape((-1,) + (1,) * (len(dims) - 1 - dim))
    return gain


def noise(own_key, extent, spread, bound, cuts=(), kind=jnp.bfloat16):
    result = jax.random.normal(own_key, extent, jnp.float32) * spread
    if len(cuts) > 0:
        result = block_levels(own_key, extent, cuts, -0.22, 0.18) * result
    return jnp.clip(result, min=-bound, max=bound).astype(kind)


def setup_inputs(seed: int = 0) -> dict:
    streams_of = jax.random.split(jax.random.key(seed), 12)
    features = noise(streams_of[0], (D, NODES), 0.5, 3.0, ((0, 4), (1, 8)))
    send_blocks = draw_send_blocks(jax.random.fold_in(streams_of[11], 71), 0)
    counts = draw_counts(jax.random.fold_in(streams_of[11], 71), 0)
    tile_blocks = draw_tile_blocks(jax.random.fold_in(streams_of[11], 71), 0)
    neighbours = set_ends(jax.random.randint(streams_of[4], (NEIGH, NODES), 0, BLOCK), jax.random.fold_in(streams_of[4], 1), 0, BLOCK - 1).astype(jnp.int32)
    degree = set_ends(jax.random.randint(streams_of[5], (NODES,), 1, NEIGH + 1), jax.random.fold_in(streams_of[5], 1), 1, NEIGH).astype(jnp.int32)
    epsilon = jnp.clip(jax.random.uniform(streams_of[6], (1,), jnp.float32, -0.3, 0.6), -0.3, 0.6)
    w_first = noise(streams_of[7], (D, H), D ** -0.5, 0.25)
    b_first = noise(streams_of[8], (H,), 0.5, 3.0, (), jnp.float32)
    w_second = noise(streams_of[9], (H, D), H ** -0.5, 0.25)
    b_second = noise(streams_of[10], (D,), 0.5, 3.0, (), jnp.float32)
    return {"features": features, "send_blocks": send_blocks, "counts": counts, "tile_blocks": tile_blocks, "neighbours": neighbours, "degree": degree, "epsilon": epsilon, "w_first": w_first, "b_first": b_first, "w_second": w_second, "b_second": b_second}


def reference(features, send_blocks, counts, tile_blocks, neighbours, degree, epsilon, w_first, b_first, w_second, b_second):
    node_rows = features.T
    tile_rows = jnp.repeat(tile_blocks.T, BLOCK, axis=0)
    lists = (tile_rows * BLOCK + neighbours.T).astype(jnp.int32)
    row_ids = jnp.arange(NODES, dtype=jnp.int32)
    row_part = (row_ids // ROWS)[:, None]
    offset = jnp.maximum(lists - ROWS, 0)
    source = offset // (SLOTS * BLOCK)
    slot_index = (offset // BLOCK) % SLOTS
    in_block = offset % BLOCK
    block_index = send_blocks[source, row_part, slot_index]
    remote = source * ROWS + block_index * BLOCK + in_block
    is_local = lists < ROWS
    target = jnp.where(is_local, row_part * ROWS + lists, remote).astype(jnp.int32)
    live_mask = (jnp.arange(NEIGH, dtype=jnp.int32)[None, :] < degree[:, None]) & (is_local | (slot_index < counts[source, row_part]))
    weight = live_mask.astype(jnp.float32)
    block_rows = min(NODES, 4096)

    def block_sum(pair):
        gathered = node_rows[pair[0]].astype(jnp.float32)
        return jnp.einsum('rk,rkd->rd', pair[1], gathered)

    near_sum = lax.map(block_sum, (target.reshape(-1, block_rows, NEIGH), weight.reshape(-1, block_rows, NEIGH)))
    near_sum = near_sum.reshape(NODES, D)
    combined = ((1.0 + epsilon[0]) * node_rows.astype(jnp.float32) + near_sum).astype(jnp.bfloat16)
    pre_act = jnp.dot(combined, w_first, preferred_element_type=jnp.float32) + b_first
    activated = jax.nn.relu(pre_act).astype(jnp.bfloat16)
    return (jnp.dot(activated, w_second, preferred_element_type=jnp.float32) + b_second).astype(jnp.bfloat16)
```

```python
import functools

import jax
import jax.numpy as jnp
from jax import lax
from jax.experimental import pallas as pl
from jax.experimental.pallas import tpu as pltpu
from jax.sharding import PartitionSpec as P

BLOCK = 128
CHUNKS = 4
NODE_TILE = 256


def kernel(
    parts, groups, chunks,
    sb_ref, cnt_ref, tile_ref, eps_ref,
    feat_ref, nbr_ref, deg_ref, w1_ref, b1_ref, w2_ref, b2_ref,
    out_ref,
    *scratch,
):
    tables = scratch[:chunks]
    local, stage, zstage, parcel, hsend, hrecv, zsend, zrecv = scratch[chunks:]
    me = lax.axis_index("dom")
    z = lax.axis_index("feat")
    slots = stage.shape[2]
    width = tables[0].shape[1]
    list_width, block_count = tile_ref.shape
    per_group = block_count // groups
    half = groups // 2

    def lanes(block):
        return pl.ds(pl.multiple_of(block * BLOCK, BLOCK), BLOCK)

    def halo_copy(c, peer, source):
        return pltpu.make_async_remote_copy(
            src_ref=stage.at[c, peer],
            dst_ref=tables[c].at[pl.ds(block_count + source * slots, slots)],
            send_sem=hsend.at[c, peer],
            recv_sem=hrecv.at[c, source],
            device_id={"dom": peer},
            device_id_type=pl.DeviceIdType.MESH,
        )

    def row_copy(c, dest, source):
        return pltpu.make_async_remote_copy(
            src_ref=zstage.at[c, dest],
            dst_ref=parcel.at[source, c],
            send_sem=zsend.at[c, dest],
            recv_sem=zrecv.at[c, source],
            device_id={"feat": dest},
            device_id_type=pl.DeviceIdType.MESH,
        )

    def dest_of(k):
        if k < half:
            return lax.rem(z // half + 1, 2) * half + lax.rem(lax.rem(z, half) + k, half)
        return (z // half) * half + lax.rem(lax.rem(z, half) + (k - half + 1), half)

    @pl.loop(0, block_count)
    def _(b):
        for c in range(chunks):
            block = feat_ref[pl.ds(c * width, width), lanes(b)]
            local[b, c] = block
            tables[c][b] = block

    barrier = pltpu.get_barrier_semaphore()

    @pl.loop(1, parts)
    def _(k):
        pl.semaphore_signal(
            barrier, inc=1, device_id={"dom": lax.rem(me + k, parts)},
            device_id_type=pl.DeviceIdType.MESH,
        )

    @pl.loop(1, groups)
    def _(k):
        pl.semaphore_signal(
            barrier, inc=1, device_id={"feat": lax.rem(z + k, groups)},
            device_id_type=pl.DeviceIdType.MESH,
        )

    pl.semaphore_wait(barrier, parts + groups - 2)

    for c in range(chunks):
        @pl.loop(1, parts)
        def _(k):
            peer = lax.rem(me + k, parts)
            for s in range(slots):
                used = (s < cnt_ref[0, peer]).astype(jnp.float32)
                block = local[sb_ref[0, peer, s], c]
                stage[c, peer, s] = (block.astype(jnp.float32) * used).astype(jnp.bfloat16)
            halo_copy(c, peer, me).start()

    for c in range(chunks):
        tables[c][pl.ds(block_count + me * slots, slots)] = jnp.zeros(
            (slots, width, BLOCK), jnp.bfloat16
        )

    gain = 1.0 + eps_ref[0]

    def mixed_block(c, b):
        total = gain * feat_ref[pl.ds(c * width, width), lanes(b)].astype(jnp.float32)
        near = jnp.zeros((width, BLOCK), jnp.float32)
        degree = deg_ref[pl.ds(b, 1), :]
        for j in range(list_width):
            tile = tables[c][tile_ref[j, b]].astype(jnp.float32)
            index = jnp.broadcast_to(nbr_ref[pl.ds(j, 1), lanes(b)], (width, BLOCK))
            taken = jnp.take_along_axis(tile, index, axis=1, mode="promise_in_bounds")
            live = jnp.broadcast_to(degree, (width, BLOCK)) > j
            near = near + jnp.where(live, taken, 0.0)
        return (total + near).astype(jnp.bfloat16)

    for c in range(chunks):
        @pl.loop(1, parts)
        def _(k):
            source = lax.rem(me + k, parts)
            halo_copy(c, source, source).wait_recv()

        for k in range(groups):
            dest = dest_of(k) if k < groups - 1 else z

            @pl.loop(0, per_group)
            def _(i):
                block = mixed_block(c, dest * per_group + i)
                if k < groups - 1:
                    zstage[c, dest, :, lanes(i)] = block
                else:
                    parcel[z, c, :, lanes(i)] = block

            if k < groups - 1:
                row_copy(c, dest, z).start()

    for c in range(chunks):
        @pl.loop(1, groups)
        def _(k):
            source = lax.rem(z + k, groups)
            row_copy(c, source, source).wait_recv()

    depth = w1_ref.shape[0]

    @pl.loop(0, out_ref.shape[0] // NODE_TILE)
    def _(n):
        nodes = pl.ds(pl.multiple_of(n * NODE_TILE, NODE_TILE), NODE_TILE)
        columns = parcel[:, :, :, nodes].reshape(depth, NODE_TILE)
        hidden = lax.dot_general(
            columns, w1_ref[...], (((0,), (0,)), ((), ())), preferred_element_type=jnp.float32
        ) + b1_ref[...]
        hidden = jnp.maximum(hidden, 0.0).astype(jnp.bfloat16)
        out_ref[nodes, :] = (
            jnp.dot(hidden, w2_ref[...], preferred_element_type=jnp.float32) + b2_ref[...]
        ).astype(jnp.bfloat16)

    for c in range(chunks):
        @pl.loop(1, parts)
        def _(k):
            halo_copy(c, lax.rem(me + k, parts), me).wait_send()

        @pl.loop(1, groups)
        def _(k):
            row_copy(c, lax.rem(z + k, groups), z).wait_send()


def per_device(
    features, send_blocks, counts, tile_blocks, neighbours, degree, epsilon,
    w_first, b_first, w_second, b_second,
):
    parts = lax.axis_size("dom")
    groups = lax.axis_size("feat")
    cols, rows = features.shape
    slots = send_blocks.shape[2]
    chunks = CHUNKS
    width = cols // chunks
    block_count = rows // BLOCK
    owned = rows // groups
    out_cols = w_second.shape[1]
    vmem = pl.BlockSpec(memory_space=pltpu.VMEM)
    smem = pl.BlockSpec(memory_space=pltpu.SMEM)
    return pl.pallas_call(
        functools.partial(kernel, parts, groups, chunks),
        out_shape=jax.ShapeDtypeStruct((owned, out_cols), jnp.bfloat16),
        in_specs=[smem] * 4 + [vmem] * 7,
        out_specs=vmem,
        scratch_shapes=[
            pltpu.VMEM((block_count + parts * slots, width, BLOCK), jnp.bfloat16)
            for _ in range(chunks)
        ] + [
            pltpu.VMEM((block_count, chunks, width, BLOCK), jnp.bfloat16),
            pltpu.VMEM((chunks, parts, slots, width, BLOCK), jnp.bfloat16),
            pltpu.VMEM((chunks, groups, width, owned), jnp.bfloat16),
            pltpu.VMEM((groups, chunks, width, owned), jnp.bfloat16),
            pltpu.SemaphoreType.DMA((chunks, parts)),
            pltpu.SemaphoreType.DMA((chunks, parts)),
            pltpu.SemaphoreType.DMA((chunks, groups)),
            pltpu.SemaphoreType.DMA((chunks, groups)),
        ],
        compiler_params=pltpu.CompilerParams(
            collective_id=0, has_side_effects=True, vmem_limit_bytes=56 * 1024 * 1024
        ),
    )(
        send_blocks, counts, tile_blocks, epsilon,
        features, neighbours, degree.reshape(block_count, BLOCK),
        w_first, b_first.reshape(1, -1), w_second, b_second.reshape(1, -1),
    )


def solution(mesh):
    return jax.shard_map(
        per_device,
        mesh=mesh,
        in_specs=(
            P("feat", "dom"),
            P("dom", None, None),
            P("dom", None),
            P(None, "dom"),
            P(None, "dom"),
            P("dom"),
            P(), P(), P(), P(), P(),
        ),
        out_specs=P(("dom", "feat"), None),
        check_vma=False,
    )
```

```python
import functools

import jax
import jax.numpy as jnp
from jax import lax
from jax.experimental import pallas as pl
from jax.experimental.pallas import tpu as pltpu
from jax.sharding import PartitionSpec as P

BLOCK = 128
SUBLANES = 16
PIECES = 4


def chunk_widths(cols):
    widths = []
    while sum(widths) < cols:
        widths.append(min(max(SUBLANES, sum(widths)), cols - sum(widths)))
    return widths


def kernel(
    parts, groups, pieces, widths,
    sb_ref, cnt_ref, tile_ref, eps_ref, deg_ref, b1_ref, b2_ref,
    feat_hbm, nbr_hbm, w1_hbm, w2_hbm,
    out_hbm,
    *scratch,
):
    chunks = len(widths)
    starts = [sum(widths[:c]) for c in range(chunks)]
    tables, locals_, stages, feats = (scratch[i * chunks:(i + 1) * chunks] for i in range(4))
    (nbr_ref, w1_ref, w2_ref, out_ref, zstage, parcel,
     hsend, hrecv, zsend, zrecv, in_sem, out_sem) = scratch[4 * chunks:]
    me = lax.axis_index("dom")
    z = lax.axis_index("feat")
    slots = stages[0].shape[1]
    list_width, block_count = tile_ref.shape
    per_piece = block_count // groups // pieces
    piece_nodes = per_piece * BLOCK
    half = groups // 2

    def lanes(block):
        return pl.ds(pl.multiple_of(block * BLOCK, BLOCK), BLOCK)

    def halo_copy(c, peer, source):
        return pltpu.make_async_remote_copy(
            src_ref=stages[c].at[peer],
            dst_ref=tables[c].at[pl.ds(block_count + source * slots, slots)],
            send_sem=hsend.at[c, peer],
            recv_sem=hrecv.at[c, source],
            device_id={"dom": peer},
            device_id_type=pl.DeviceIdType.MESH,
        )

    def row_copy(c, p, dest, source):
        span = pl.ds(starts[c], widths[c])
        return pltpu.make_async_remote_copy(
            src_ref=zstage.at[p, dest, span],
            dst_ref=parcel.at[p, source, span],
            send_sem=zsend.at[c, p, dest],
            recv_sem=zrecv.at[c, p, source],
            device_id={"feat": dest},
            device_id_type=pl.DeviceIdType.MESH,
        )

    def dest_of(k):
        if k < half:
            return lax.rem(z // half + 1, 2) * half + lax.rem(lax.rem(z, half) + k, half)
        return (z // half) * half + lax.rem(lax.rem(z, half) + (k - half + 1), half)

    barrier = pltpu.get_barrier_semaphore()

    @pl.loop(1, parts)
    def _(k):
        pl.semaphore_signal(
            barrier, inc=1, device_id={"dom": lax.rem(me + k, parts)},
            device_id_type=pl.DeviceIdType.MESH,
        )

    @pl.loop(1, groups)
    def _(k):
        pl.semaphore_signal(
            barrier, inc=1, device_id={"feat": lax.rem(z + k, groups)},
            device_id_type=pl.DeviceIdType.MESH,
        )

    loads = [
        pltpu.make_async_copy(
            feat_hbm.at[pl.ds(starts[c], widths[c])], feats[c], in_sem.at[c]
        )
        for c in range(chunks)
    ]
    loads.append(pltpu.make_async_copy(nbr_hbm, nbr_ref, in_sem.at[chunks]))
    loads.append(pltpu.make_async_copy(w1_hbm, w1_ref, in_sem.at[chunks + 1]))
    loads.append(pltpu.make_async_copy(w2_hbm, w2_ref, in_sem.at[chunks + 2]))
    for load in loads:
        load.start()

    for c in range(chunks):
        loads[c].wait()

        @pl.loop(0, block_count, unroll=4)
        def _(b):
            block = feats[c][:, lanes(b)]
            locals_[c][b] = block
            tables[c][b] = block

        if c == 0:
            pl.semaphore_wait(barrier, parts + groups - 2)

        @pl.loop(1, parts)
        def _(k):
            peer = lax.rem(me + k, parts)
            for s in range(slots):
                used = (s < cnt_ref[0, peer]).astype(jnp.float32)
                block = locals_[c][sb_ref[0, peer, s]]
                stages[c][peer, s] = (block.astype(jnp.float32) * used).astype(jnp.bfloat16)
            halo_copy(c, peer, me).start()

    for c in range(chunks):
        tables[c][pl.ds(block_count + me * slots, slots)] = jnp.zeros(
            (slots, widths[c], BLOCK), jnp.bfloat16
        )

    gain = 1.0 + eps_ref[0]
    loads[chunks].wait()

    def mixed_block(c, b):
        shape = (widths[c], BLOCK)
        total = gain * feats[c][:, lanes(b)].astype(jnp.float32)
        near = jnp.zeros(shape, jnp.float32)
        degree = jnp.broadcast_to(deg_ref[pl.ds(b, 1), :], shape)
        for j in range(list_width):
            tile = tables[c][tile_ref[j, b]].astype(jnp.float32)
            index = jnp.broadcast_to(nbr_ref[pl.ds(j, 1), lanes(b)], shape)
            taken = jnp.take_along_axis(tile, index, axis=1, mode="promise_in_bounds")
            near = near + jnp.where(degree > j, taken, 0.0)
        return (total + near).astype(jnp.bfloat16)

    for c in range(chunks):
        @pl.loop(1, parts)
        def _(k):
            source = lax.rem(me + k, parts)
            halo_copy(c, source, source).wait_recv()

        span = pl.ds(starts[c], widths[c])
        unroll = per_piece if widths[c] <= 2 * SUBLANES else max(per_piece // 2, 1)

        @pl.loop(0, pieces)
        def _(p):
            for k in range(groups):
                dest = dest_of(k) if k < groups - 1 else z
                first = (dest * pieces + p) * per_piece

                @pl.loop(0, per_piece, unroll=unroll)
                def _(i):
                    block = mixed_block(c, first + i)
                    if k < groups - 1:
                        zstage[p, dest, span, lanes(i)] = block
                    else:
                        parcel[p, z, span, lanes(i)] = block

                if k < groups - 1:
                    row_copy(c, p, dest, z).start()

    loads[chunks + 1].wait()
    loads[chunks + 2].wait()
    depth = w1_ref.shape[0]

    def out_copy(p):
        rows = pl.ds(pl.multiple_of(p * piece_nodes, piece_nodes), piece_nodes)
        return pltpu.make_async_copy(out_ref.at[rows], out_hbm.at[rows], out_sem.at[p])

    @pl.loop(0, pieces)
    def _(p):
        for c in range(chunks):
            @pl.loop(1, groups)
            def _(k):
                source = lax.rem(z + k, groups)
                row_copy(c, p, source, source).wait_recv()

        columns = parcel[p].reshape(depth, piece_nodes)
        hidden = lax.dot_general(
            columns, w1_ref[...], (((0,), (0,)), ((), ())), preferred_element_type=jnp.float32
        ) + b1_ref[...]
        hidden = jnp.maximum(hidden, 0.0).astype(jnp.bfloat16)
        rows = pl.ds(pl.multiple_of(p * piece_nodes, piece_nodes), piece_nodes)
        out_ref[rows, :] = (
            jnp.dot(hidden, w2_ref[...], preferred_element_type=jnp.float32) + b2_ref[...]
        ).astype(jnp.bfloat16)
        out_copy(p).start()

    for c in range(chunks):
        @pl.loop(1, parts)
        def _(k):
            halo_copy(c, lax.rem(me + k, parts), me).wait_send()

        @pl.loop(0, pieces)
        def _(p):
            @pl.loop(1, groups)
            def _(k):
                row_copy(c, p, lax.rem(z + k, groups), z).wait_send()

    @pl.loop(0, pieces)
    def _(p):
        out_copy(p).wait()


def per_device(
    features, send_blocks, counts, tile_blocks, neighbours, degree, epsilon,
    w_first, b_first, w_second, b_second,
):
    parts = lax.axis_size("dom")
    groups = lax.axis_size("feat")
    cols, rows = features.shape
    slots = send_blocks.shape[2]
    widths = chunk_widths(cols)
    chunks = len(widths)
    block_count = rows // BLOCK
    owned = rows // groups
    pieces = min(PIECES, owned // BLOCK)
    hidden_cols, out_cols = w_second.shape
    depth = w_first.shape[0]
    vmem = pl.BlockSpec(memory_space=pltpu.VMEM)
    smem = pl.BlockSpec(memory_space=pltpu.SMEM)
    anywhere = pl.BlockSpec(memory_space=pl.ANY)
    bf16 = jnp.bfloat16
    return pl.pallas_call(
        functools.partial(kernel, parts, groups, pieces, widths),
        out_shape=jax.ShapeDtypeStruct((owned, out_cols), bf16),
        in_specs=[smem] * 4 + [vmem] * 3 + [anywhere] * 4,
        out_specs=anywhere,
        scratch_shapes=[
            pltpu.VMEM((block_count + parts * slots, w, BLOCK), bf16) for w in widths
        ] + [
            pltpu.VMEM((block_count, w, BLOCK), bf16) for w in widths
        ] + [
            pltpu.VMEM((parts, slots, w, BLOCK), bf16) for w in widths
        ] + [
            pltpu.VMEM((w, rows), bf16) for w in widths
        ] + [
            pltpu.VMEM(neighbours.shape, jnp.int32),
            pltpu.VMEM((depth, hidden_cols), bf16),
            pltpu.VMEM((hidden_cols, out_cols), bf16),
            pltpu.VMEM((owned, out_cols), bf16),
            pltpu.VMEM((pieces, groups, cols, owned // pieces), bf16),
            pltpu.VMEM((pieces, groups, cols, owned // pieces), bf16),
            pltpu.SemaphoreType.DMA((chunks, parts)),
            pltpu.SemaphoreType.DMA((chunks, parts)),
            pltpu.SemaphoreType.DMA((chunks, pieces, groups)),
            pltpu.SemaphoreType.DMA((chunks, pieces, groups)),
            pltpu.SemaphoreType.DMA((chunks + 3,)),
            pltpu.SemaphoreType.DMA((pieces,)),
        ],
        compiler_params=pltpu.CompilerParams(
            collective_id=0, has_side_effects=True, vmem_limit_bytes=56 * 1024 * 1024
        ),
    )(
        send_blocks, counts, tile_blocks, epsilon,
        degree.reshape(block_count, BLOCK), b_first.reshape(1, -1), b_second.reshape(1, -1),
        features, neighbours, w_first, w_second,
    )


def solution(mesh):
    return jax.shard_map(
        per_device,
        mesh=mesh,
        in_specs=(
            P("feat", "dom"),
            P("dom", None, None),
            P("dom", None),
            P(None, "dom"),
            P(None, "dom"),
            P("dom"),
            P(), P(), P(), P(), P(),
        ),
        out_specs=P(("dom", "feat"), None),
        check_vma=False,
    )
```

```python
import functools

import jax
import jax.numpy as jnp
from jax import lax
from jax.experimental import pallas as pl
from jax.experimental.pallas import tpu as pltpu
from jax.sharding import PartitionSpec as P

BLOCK = 128
SUBLANES = 16
PIECES = 4


def chunk_widths(cols):
    widths = []
    while sum(widths) < cols:
        widths.append(min(max(SUBLANES, sum(widths)), cols - sum(widths)))
    return widths


def kernel(
    parts, groups, pieces, widths,
    sb_ref, cnt_ref, tile_ref, eps_ref, deg_ref, b1_ref, b2_ref,
    feat_hbm, nbr_hbm, w1_hbm, w2_hbm,
    out_ref,
    *scratch,
):
    chunks = len(widths)
    starts = [sum(widths[:c]) for c in range(chunks)]
    tables, locals_, stages, feats = (scratch[i * chunks:(i + 1) * chunks] for i in range(4))
    (nbr_ref, w1_ref, w2_ref, zstage, parcel,
     hsend, hrecv, zsend, zrecv, in_sem) = scratch[4 * chunks:]
    me = lax.axis_index("dom")
    z = lax.axis_index("feat")
    slots = stages[0].shape[1]
    list_width, block_count = tile_ref.shape
    per_piece = block_count // groups // pieces
    piece_nodes = per_piece * BLOCK
    half = groups // 2

    def lanes(block):
        return pl.ds(pl.multiple_of(block * BLOCK, BLOCK), BLOCK)

    def halo_copy(c, peer, source):
        return pltpu.make_async_remote_copy(
            src_ref=stages[c].at[peer],
            dst_ref=tables[c].at[pl.ds(block_count + source * slots, slots)],
            send_sem=hsend.at[c, peer],
            recv_sem=hrecv.at[c, source],
            device_id={"dom": peer},
            device_id_type=pl.DeviceIdType.MESH,
        )

    def row_copy(c, p, dest, source):
        span = pl.ds(starts[c], widths[c])
        return pltpu.make_async_remote_copy(
            src_ref=zstage.at[p, dest, span],
            dst_ref=parcel.at[p, source, span],
            send_sem=zsend.at[c, p, dest],
            recv_sem=zrecv.at[c, p, source],
            device_id={"feat": dest},
            device_id_type=pl.DeviceIdType.MESH,
        )

    def dest_of(k):
        if k < half:
            return lax.rem(z // half + 1, 2) * half + lax.rem(lax.rem(z, half) + k, half)
        return (z // half) * half + lax.rem(lax.rem(z, half) + (k - half + 1), half)

    barrier = pltpu.get_barrier_semaphore()

    @pl.loop(1, parts)
    def _(k):
        pl.semaphore_signal(
            barrier, inc=1, device_id={"dom": lax.rem(me + k, parts)},
            device_id_type=pl.DeviceIdType.MESH,
        )

    @pl.loop(1, groups)
    def _(k):
        pl.semaphore_signal(
            barrier, inc=1, device_id={"feat": lax.rem(z + k, groups)},
            device_id_type=pl.DeviceIdType.MESH,
        )

    loads = [
        pltpu.make_async_copy(
            feat_hbm.at[pl.ds(starts[c], widths[c])], feats[c], in_sem.at[c]
        )
        for c in range(chunks)
    ]
    loads.append(pltpu.make_async_copy(nbr_hbm, nbr_ref, in_sem.at[chunks]))
    loads.append(pltpu.make_async_copy(w1_hbm, w1_ref, in_sem.at[chunks + 1]))
    loads.append(pltpu.make_async_copy(w2_hbm, w2_ref, in_sem.at[chunks + 2]))
    for load in loads:
        load.start()

    for c in range(chunks):
        loads[c].wait()

        @pl.loop(0, block_count, unroll=4)
        def _(b):
            block = feats[c][:, lanes(b)]
            locals_[c][b] = block
            tables[c][b] = block

        if c == 0:
            pl.semaphore_wait(barrier, parts + groups - 2)

        @pl.loop(1, parts)
        def _(k):
            peer = lax.rem(me + k, parts)
            for s in range(slots):
                used = (s < cnt_ref[0, peer]).astype(jnp.float32)
                block = locals_[c][sb_ref[0, peer, s]]
                stages[c][peer, s] = (block.astype(jnp.float32) * used).astype(jnp.bfloat16)
            halo_copy(c, peer, me).start()

    for c in range(chunks):
        tables[c][pl.ds(block_count + me * slots, slots)] = jnp.zeros(
            (slots, widths[c], BLOCK), jnp.bfloat16
        )

    gain = 1.0 + eps_ref[0]
    loads[chunks].wait()

    def mixed_block(c, b):
        shape = (widths[c], BLOCK)
        total = gain * feats[c][:, lanes(b)].astype(jnp.float32)
        near = jnp.zeros(shape, jnp.float32)
        degree = jnp.broadcast_to(deg_ref[pl.ds(b, 1), :], shape)
        for j in range(list_width):
            tile = tables[c][tile_ref[j, b]].astype(jnp.float32)
            index = jnp.broadcast_to(nbr_ref[pl.ds(j, 1), lanes(b)], shape)
            taken = jnp.take_along_axis(tile, index, axis=1, mode="promise_in_bounds")
            near = near + jnp.where(degree > j, taken, 0.0)
        return (total + near).astype(jnp.bfloat16)

    for c in range(chunks):
        @pl.loop(1, parts)
        def _(k):
            source = lax.rem(me + k, parts)
            halo_copy(c, source, source).wait_recv()

        span = pl.ds(starts[c], widths[c])
        unroll = per_piece if widths[c] <= 2 * SUBLANES else max(per_piece // 2, 1)

        @pl.loop(0, pieces)
        def _(p):
            for k in range(groups):
                dest = dest_of(k) if k < groups - 1 else z
                first = (dest * pieces + p) * per_piece

                @pl.loop(0, per_piece, unroll=unroll)
                def _(i):
                    block = mixed_block(c, first + i)
                    if k < groups - 1:
                        zstage[p, dest, span, lanes(i)] = block
                    else:
                        parcel[p, z, span, lanes(i)] = block

                if k < groups - 1:
                    row_copy(c, p, dest, z).start()

    loads[chunks + 1].wait()
    loads[chunks + 2].wait()
    depth = w1_ref.shape[0]

    @pl.loop(0, pieces)
    def _(p):
        for c in range(chunks):
            @pl.loop(1, groups)
            def _(k):
                source = lax.rem(z + k, groups)
                row_copy(c, p, source, source).wait_recv()

        columns = parcel[p].reshape(depth, piece_nodes)
        hidden = lax.dot_general(
            columns, w1_ref[...], (((0,), (0,)), ((), ())), preferred_element_type=jnp.float32
        ) + b1_ref[...]
        hidden = jnp.maximum(hidden, 0.0).astype(jnp.bfloat16)
        rows = pl.ds(pl.multiple_of(p * piece_nodes, piece_nodes), piece_nodes)
        out_ref[rows, :] = (
            jnp.dot(hidden, w2_ref[...], preferred_element_type=jnp.float32) + b2_ref[...]
        ).astype(jnp.bfloat16)

    for c in range(chunks):
        @pl.loop(1, parts)
        def _(k):
            halo_copy(c, lax.rem(me + k, parts), me).wait_send()

        @pl.loop(0, pieces)
        def _(p):
            @pl.loop(1, groups)
            def _(k):
                row_copy(c, p, lax.rem(z + k, groups), z).wait_send()


def per_device(
    features, send_blocks, counts, tile_blocks, neighbours, degree, epsilon,
    w_first, b_first, w_second, b_second,
):
    parts = lax.axis_size("dom")
    groups = lax.axis_size("feat")
    cols, rows = features.shape
    slots = send_blocks.shape[2]
    widths = chunk_widths(cols)
    chunks = len(widths)
    block_count = rows // BLOCK
    owned = rows // groups
    pieces = min(PIECES, owned // BLOCK)
    hidden_cols, out_cols = w_second.shape
    depth = w_first.shape[0]
    vmem = pl.BlockSpec(memory_space=pltpu.VMEM)
    smem = pl.BlockSpec(memory_space=pltpu.SMEM)
    anywhere = pl.BlockSpec(memory_space=pl.ANY)
    bf16 = jnp.bfloat16
    return pl.pallas_call(
        functools.partial(kernel, parts, groups, pieces, widths),
        out_shape=pltpu.VMEM((owned, out_cols), bf16),
        in_specs=[smem] * 4 + [vmem] * 3 + [anywhere] * 4,
        out_specs=vmem,
        scratch_shapes=[
            pltpu.VMEM((block_count + parts * slots, w, BLOCK), bf16) for w in widths
        ] + [
            pltpu.VMEM((block_count, w, BLOCK), bf16) for w in widths
        ] + [
            pltpu.VMEM((parts, slots, w, BLOCK), bf16) for w in widths
        ] + [
            pltpu.VMEM((w, rows), bf16) for w in widths
        ] + [
            pltpu.VMEM(neighbours.shape, jnp.int32),
            pltpu.VMEM((depth, hidden_cols), bf16),
            pltpu.VMEM((hidden_cols, out_cols), bf16),
            pltpu.VMEM((pieces, groups, cols, owned // pieces), bf16),
            pltpu.VMEM((pieces, groups, cols, owned // pieces), bf16),
            pltpu.SemaphoreType.DMA((chunks, parts)),
            pltpu.SemaphoreType.DMA((chunks, parts)),
            pltpu.SemaphoreType.DMA((chunks, pieces, groups)),
            pltpu.SemaphoreType.DMA((chunks, pieces, groups)),
            pltpu.SemaphoreType.DMA((chunks + 3,)),
        ],
        compiler_params=pltpu.CompilerParams(
            collective_id=0, has_side_effects=True, vmem_limit_bytes=56 * 1024 * 1024
        ),
    )(
        send_blocks, counts, tile_blocks, epsilon,
        degree.reshape(block_count, BLOCK), b_first.reshape(1, -1), b_second.reshape(1, -1),
        features, neighbours, w_first, w_second,
    )


def solution(mesh):
    return jax.shard_map(
        per_device,
        mesh=mesh,
        in_specs=(
            P("feat", "dom"),
            P("dom", None, None),
            P("dom", None),
            P(None, "dom"),
            P(None, "dom"),
            P("dom"),
            P(), P(), P(), P(), P(),
        ),
        out_specs=P(("dom", "feat"), None),
        check_vma=False,
    )
```
